32 devices in a mesh: freq: 4 (over z), trace: 8 (over y, x, core).
Axes of the slice: x: 2, y: 2, z: 4, core: 2. Of those that a mesh axis runs over, the one named last changes fastest.
Arguments:
- recorded: float32 [8, 2, 2048, 1024], P(None, None, 'freq', 'trace'), may hold values from -16 to 16
- multiples: float32 [8, 2, 2048, 1024], P(None, None, 'freq', 'trace'), may hold values from -6 to 6
Outputs:
- primaries: float32 [8, 2, 2048, 1024], P(None, None, 'freq', 'trace')
- filters: float32 [8, 2, 32, 64], P(None, None, 'freq')
The draws below stay inside these ranges and needn't reach their ends.
All inputs are finite; a program needn't handle non-finite values.
Results may differ from the reference program's by a relative error of at most 0.0001.
Values sent between devices are 32-bit elements; how exact they have to be, the bound alone decides.
A program may use at most 128 MiB of HBM per device.

```python
import jax
import jax.numpy as jnp
from jax import lax

SHOTS = 8
NF = 2048
FB = 64
TAPS = 64
ITERS = 3
NX = 1024
NB = 32
N_TRACE = 8


def paired_fields(key):
    key_mult, key_smooth, key_noise, key_first, key_second = jax.random.split(jax.random.fold_in(key, 17), 5)
    white_part = jax.random.normal(key_mult, (SHOTS, 2, NF, NX), jnp.float32)
    base_field = jax.random.normal(key_smooth, (SHOTS, 2, NF, NX), jnp.float32)
    smooth_part = base_field
    for offset in range(1, 12):
        smooth_part = smooth_part + jnp.roll(base_field, offset, axis=3)
    smooth_part = smooth_part * 0.28867513
    mult_field = jnp.clip((white_part + 2.0 * smooth_part) * 0.4472136, -6.0, 6.0)
    noise_part = jnp.clip(jax.random.normal(key_noise, (SHOTS, 2, NF, NX), jnp.float32), -4.0, 4.0)
    first_gain = jax.random.uniform(key_first, (SHOTS, 2, NF, 1), jnp.float32, -1.0, 1.0)
    second_gain = jax.random.uniform(key_second, (SHOTS, 2, NF, 1), jnp.float32, -0.6, 0.6)
    shifted = jnp.roll(mult_field, 1, axis=3)
    real_part = first_gain[:, 0] * mult_field[:, 0] - first_gain[:, 1] * mult_field[:, 1] + second_gain[:, 0] * shifted[:, 0] - second_gain[:, 1] * shifted[:, 1]
    imag_part = first_gain[:, 0] * mult_field[:, 1] + first_gain[:, 1] * mult_field[:, 0] + second_gain[:, 0] * shifted[:, 1] + second_gain[:, 1] * shifted[:, 0]
    recorded_field = jnp.clip(noise_part + jnp.stack([real_part, imag_part], axis=1), -16.0, 16.0)
    return (recorded_field, mult_field)


def draw_recorded(key, part):
    return paired_fields(key)[0]


def draw_multiples(key, part):
    return paired_fields(key)[1]


def setup_inputs(seed: int = 0) -> dict:
    key_of = jax.random.split(jax.random.key(seed), 3)
    recorded = draw_recorded(jax.random.fold_in(key_of[2], 71), 0)
    multiples = draw_multiples(jax.random.fold_in(key_of[2], 71), 0)
    return dict(recorded=recorded, multiples=multiples)


def toeplitz_rows(taps_vec, trace_rows):
    tap_count = taps_vec.shape[-1]
    window_len = trace_rows + tap_count
    leading = taps_vec.shape[:-1]
    padded = jnp.concatenate([jnp.zeros(leading + (1,), jnp.float32), taps_vec[..., ::-1], jnp.zeros(leading + (trace_rows,), jnp.float32)], -1)
    repeated = jnp.tile(padded, (1,) * len(leading) + (trace_rows,))
    return repeated[..., :trace_rows * window_len].reshape(leading + (trace_rows, window_len))


def product(left, right):
    return jnp.einsum('bfj,bxj->bfx', left, right, precision=lax.Precision.HIGHEST)


def correlate(left, right):
    return jnp.einsum('bfj,bfx->bxj', left, right, precision=lax.Precision.HIGHEST)


def forward_one(window, taps_vec):
    trace_rows = window.shape[-1] - taps_vec.shape[-1]
    toeplitz = toeplitz_rows(taps_vec, trace_rows)
    real_part = product(window[0], toeplitz[0]) - product(window[1], toeplitz[1])
    imag_part = product(window[0], toeplitz[1]) + product(window[1], toeplitz[0])
    return jnp.stack([real_part, imag_part])


def adjoint_one(window, residual, tap_count):
    real_part = correlate(window[0], residual[0]) + correlate(window[1], residual[1])
    imag_part = correlate(window[0], residual[1]) - correlate(window[1], residual[0])
    crossed = jnp.stack([real_part, imag_part])
    trace_rows, window_len = crossed.shape[-2:]
    leading = crossed.shape[:-2]
    flattened = crossed.reshape(leading + (trace_rows * window_len,))
    flattened = jnp.concatenate([flattened, jnp.zeros(leading + (trace_rows,), jnp.float32)], -1)
    column_sums = jnp.sum(flattened.reshape(leading + (trace_rows, window_len + 1)), axis=-2)
    return column_sums[..., 1:tap_count + 1][..., ::-1]


def reference(recorded, multiples):
    half_taps = TAPS // 2
    tile_rows = NX // N_TRACE
    window_len = tile_rows + TAPS
    padded = jnp.pad(multiples, ((0, 0), (0, 0), (0, 0), (half_taps, half_taps)))
    tiles_all = jnp.stack([padded[..., tile_index * tile_rows: tile_index * tile_rows + window_len] for tile_index in range(N_TRACE)])
    tiles_all = tiles_all.reshape(N_TRACE, SHOTS, 2, NB, FB, window_len)
    weight = 0.5 * FB * NX

    def forward(shaping):
        result = lax.map(lambda tile: lax.map(lambda paired: forward_one(paired[0], paired[1]), (tile, shaping)), tiles_all)
        return jnp.moveaxis(result, 0, 4).reshape(SHOTS, 2, NF, NX)

    def adjoint(residual):
        pieces = jnp.moveaxis(residual.reshape(SHOTS, 2, NB, FB, N_TRACE, tile_rows), 4, 0)
        result = lax.map(lambda paired: lax.map(lambda inner_pair: adjoint_one(inner_pair[0], inner_pair[1], TAPS), paired), (tiles_all, pieces))
        return jnp.sum(result, axis=0)

    def bending(vector):
        edge_pad = jnp.pad(vector, ((0, 0), (0, 0), (1, 1), (0, 0)))
        return 2.0 * vector - edge_pad[:, :, :-2] - edge_pad[:, :, 2:]

    def inner_sum(left, right):
        return jnp.sum(left * right, axis=(1, 2, 3))

    shaping = jnp.zeros((SHOTS, 2, NB, TAPS), jnp.float32)
    bent_sum = jnp.zeros((SHOTS, 2, NB, TAPS), jnp.float32)
    residual = recorded
    direction = shaping
    norm_now = jnp.ones((SHOTS,), jnp.float32)
    for iteration in range(ITERS):
        gradient = adjoint(residual) - bent_sum
        norm_next = inner_sum(gradient, gradient)
        if iteration == 0:
            direction = gradient
        else:
            direction = gradient + (norm_next / norm_now)[:, None, None, None] * direction
        norm_now = norm_next
        applied = forward(direction)
        smooth = weight * bending(direction)
        energy = inner_sum(applied, applied) + inner_sum(direction, smooth)
        step_len = (norm_now / energy)[:, None, None, None]
        shaping = shaping + step_len * direction
        residual = residual - step_len * applied
        bent_sum = bent_sum + step_len * smooth
    return residual, shaping
```

```python
import functools

import jax
import jax.numpy as jnp
from jax import lax
from jax.experimental import pallas as pl
from jax.experimental.pallas import tpu as pltpu
from jax.sharding import PartitionSpec as P

FB = 64
TAPS = 64
ITERS = 3
HALF = TAPS // 2
LANES = 128
ROWS = 4 + HALF
F32 = jnp.float32
BF16 = jnp.bfloat16


def lanes_of(shape):
    return lax.broadcasted_iota(jnp.int32, shape, len(shape) - 1)


def turn(value, shift):
    shift = shift % LANES
    return value if shift == 0 else pltpu.roll(value, shift, 1)


def split(value):
    high = value.astype(BF16)
    return high, (value - high.astype(F32)).astype(BF16)


def tiles(m_ref, left_ref, right_ref, b, part):
    group_rows = left_ref.shape[2]
    group, first = (b * FB) // group_rows, (b * FB) % group_rows
    main = m_ref[0, part, b * FB : (b + 1) * FB, :]
    left = turn(left_ref[0, part, first : first + FB, :], LANES - HALF - HALF * group)
    right = turn(right_ref[0, part, first : first + FB, :], -HALF * group)
    lane = lanes_of(main.shape)
    halo = jnp.where(lane < HALF, right, jnp.where(lane >= LANES - HALF, left, 0.0))
    return main, halo


def three(pair):
    (rh, rl), (ih, il) = pair
    return jnp.concatenate([rh, ih, rh, ih, rl, il], 0)


def three_re(pair):
    (rh, rl), (ih, il) = pair
    return jnp.concatenate([rh, ih, rl, il, rh, ih], 0)


def three_im(pair):
    (rh, rl), (ih, il) = pair
    return jnp.concatenate([ih, -rh, il, -rl, ih, -rh], 0)


def over_first(left, right):
    return lax.dot_general(left, right, (((0,), (0,)), ((), ())), preferred_element_type=F32)


def diagonals(main, halo, offset):
    lane = lanes_of((8, LANES))
    total = jnp.zeros((8, LANES), F32)
    for g in range(LANES // 8):
        shift = offset - 8 * g
        own = turn(main[8 * g : 8 * g + 8], shift)
        other = turn(halo[8 * g : 8 * g + 8], shift)
        outside = lane < shift if shift >= 0 else lane >= LANES + shift
        total = total + jnp.where(outside, other, own)
    row = lax.broadcasted_iota(jnp.int32, (8, LANES), 0)
    result = jnp.where(row == 0, total, 0.0)
    for s in range(1, 8):
        result = result + jnp.where(row == s, turn(total, -s), 0.0)
    return jnp.sum(result, axis=0, keepdims=True)


def stats_kernel(mask_ref, m_ref, left_ref, right_ref, rec_ref, out_ref):
    for b in range(m_ref.shape[2] // FB):
        windows, starts, ends, records = [], [], [], []
        for part in range(2):
            main, halo = tiles(m_ref, left_ref, right_ref, b, part)
            turned = turn(main, HALF)
            shifted = jnp.where(lanes_of(main.shape) < HALF, turn(halo, HALF), turned)
            windows.append(split(jnp.concatenate([main, halo], 1)))
            starts.append(split(jnp.concatenate([shifted, rec_ref[0, part, b * FB : (b + 1) * FB, :]], 1)))
            ends.append(split(turned))
        crossed = over_first(three(starts), jnp.concatenate([three_re(windows), three_im(windows)], 1))
        edge = over_first(three(ends)[:, :TAPS], jnp.concatenate([three_re(ends), three_im(ends)], 1))
        quads = []
        for first, offset in ((0, HALF), (LANES, HALF - 1)):
            for column in (0, 2 * LANES):
                rows = slice(first, first + LANES)
                quads.append(
                    diagonals(
                        crossed[rows, column : column + LANES],
                        crossed[rows, column + LANES : column + 2 * LANES],
                        offset,
                    )
                )
        quads[3] = -quads[3]
        real, imag = edge[:, :LANES], turn(edge[:, LANES:], TAPS)
        lane = lanes_of((HALF, LANES))
        corner = jnp.where(
            lane < HALF,
            real[:HALF],
            jnp.where(lane < TAPS, real[HALF:], jnp.where(lane < TAPS + HALF, imag[:HALF], imag[HALF:])),
        )
        corner = jnp.where(mask_ref[...] > 0.0, corner, 0.0)
        out_ref[0, :, b, :] = jnp.concatenate(quads + [corner], 0)


def exact(left, right):
    return jnp.dot(left, right, precision=lax.Precision.HIGHEST, preferred_element_type=F32)


def mirror(total):
    rows = lax.broadcasted_iota(jnp.int32, (LANES, LANES), 0)
    return (rows + lanes_of((LANES, LANES)) == total).astype(F32)


def total_of(value):
    return jnp.sum(jnp.sum(value, axis=1, keepdims=True), axis=0, keepdims=True)


def solve_kernel(weight, st_ref, out_ref, matrix):
    blocks = st_ref.shape[0] * st_ref.shape[3]

    def row(r):
        return st_ref[:, 0, r, :, :].reshape(blocks, LANES)

    lane = lanes_of((blocks, LANES))
    place = lane % TAPS
    is_real = lane < TAPS
    carry_right = place < HALF - 1
    carry_left = place > HALF
    in_right = place < HALF
    right = [None] * HALF
    for i in reversed(range(HALF)):
        value = jnp.where(in_right, row(4 + i), 0.0)
        if i + 1 < HALF:
            value = value + jnp.where(carry_right, turn(right[i + 1], -1), 0.0)
        right[i] = value
        if i >= 1:
            matrix[i - 1] = jnp.where(carry_right, turn(value, -1), 0.0)
    matrix[HALF - 1] = jnp.zeros((blocks, LANES), F32)
    last = None
    for i in range(HALF):
        value = jnp.where(in_right, 0.0, row(4 + i))
        if i:
            value = value + jnp.where(carry_left, turn(last, 1), 0.0)
        last = value
        matrix[HALF + i] = value
    lag_real = jnp.where(is_real, row(0), 0.0) + jnp.where(lane < HALF, right[0], 0.0)
    lag_imag = jnp.where(is_real, row(1), 0.0) + jnp.where(lane < HALF, turn(right[0], TAPS), 0.0)
    back = mirror(LANES)
    toep_real = jnp.where(is_real, lag_real, exact(lag_real, back))
    toep_imag = jnp.where(is_real, -lag_imag, exact(lag_imag, back))
    for t in range(TAPS):
        toep = jnp.where(is_real, turn(toep_real, t), turn(toep_imag, TAPS + t))
        matrix[t] = toep - jnp.where(is_real, matrix[t], -matrix[t])

    gradient = jnp.where(is_real, row(2), turn(row(3), TAPS))
    filters = jnp.zeros((blocks, LANES), F32)
    direction = norm_now = None
    none = jnp.zeros((1, LANES), F32)
    for iteration in range(ITERS):
        norm_next = total_of(gradient * gradient)
        if iteration == 0:
            direction = gradient
        else:
            direction = gradient + (norm_next / norm_now) * direction
        norm_now = norm_next
        by_real = jnp.zeros((blocks, LANES), F32)
        by_imag = jnp.zeros((blocks, LANES), F32)
        for t in range(TAPS):
            by_real = by_real + direction[:, t : t + 1] * matrix[t]
            by_imag = by_imag + direction[:, TAPS + t : TAPS + t + 1] * matrix[t]
        by_imag = turn(by_imag, TAPS)
        normal = by_real + jnp.where(is_real, -by_imag, by_imag)
        before = jnp.concatenate([none, direction[:-1]], 0)
        after = jnp.concatenate([direction[1:], none], 0)
        normal = normal + weight * (2.0 * direction - before - after)
        step_len = norm_now / total_of(direction * normal)
        filters = filters + step_len * direction
        gradient = gradient - step_len * normal
    out_ref[0, 0] = exact(filters, mirror(TAPS - 1))
    out_ref[0, 1] = exact(jnp.where(is_real, 0.0, filters), mirror(2 * TAPS - 1))


def forward_kernel(h_ref, m_ref, left_ref, right_ref, rec_ref, out_ref):
    rows = lax.broadcasted_iota(jnp.int32, (LANES, LANES), 0)
    tap = lanes_of((LANES, LANES)) + HALF - rows
    direct = (tap >= 0) & (tap < TAPS)
    for b in range(m_ref.shape[2] // FB):
        windows, bands = [], []
        for part in range(2):
            windows.append(split(jnp.concatenate(tiles(m_ref, left_ref, right_ref, b, part), 1)))
            base = jnp.where(lanes_of((1, LANES)) < TAPS, h_ref[0, part, b : b + 1, :], 0.0)
            base = pltpu.roll(jnp.broadcast_to(base, (8, LANES)), 0, 1, stride=1, stride_axis=0)
            ring = jnp.concatenate([turn(base, 8 * g - HALF) for g in range(LANES // 8)], 0)
            band = jnp.concatenate([jnp.where(direct, ring, 0.0), jnp.where(direct, 0.0, ring)], 0)
            bands.append(split(band))
        (rh, rl), (ih, il) = windows
        high, low = jnp.concatenate([rh, ih], 1), jnp.concatenate([rl, il], 1)
        sides = []
        for term in range(2):
            real, imag = bands[0][term], bands[1][term]
            sides.append(
                jnp.concatenate(
                    [jnp.concatenate([real, imag], 1), jnp.concatenate([-imag, real], 1)], 0
                )
            )
        both = jnp.dot(jnp.concatenate([high, low], 0), sides[0], preferred_element_type=F32)
        applied = both[:FB] + both[FB:] + jnp.dot(high, sides[1], preferred_element_type=F32)
        span = slice(b * FB, (b + 1) * FB)
        out_ref[0, 0, span, :] = rec_ref[0, 0, span, :] - applied[:, :LANES]
        out_ref[0, 1, span, :] = rec_ref[0, 1, span, :] - applied[:, LANES:]


def packed(value):
    count = LANES // HALF
    return jnp.concatenate(jnp.split(value, count, axis=2), axis=3)


def body(recorded, multiples):
    shots, parts, freq_rows, trace_rows = multiples.shape
    blocks = freq_rows // FB
    trace_count, freq_count = lax.axis_size("trace"), lax.axis_size("freq")
    me = lax.axis_index("trace")
    up = [(i, i + 1) for i in range(trace_count - 1)]
    down = [(j, i) for i, j in up]
    left = lax.ppermute(packed(multiples[..., trace_rows - HALF :]), "trace", up)
    right = lax.ppermute(packed(multiples[..., :HALF]), "trace", down)

    place = jnp.arange(LANES)[None, :] % TAPS < HALF
    mask = jnp.where(place, me == trace_count - 1, me == 0).astype(F32)

    field = pl.BlockSpec((1, parts, freq_rows, trace_rows), lambda s: (s, 0, 0, 0))
    side = pl.BlockSpec((1, parts) + left.shape[2:], lambda s: (s, 0, 0, 0))
    stats = pl.pallas_call(
        stats_kernel,
        grid=(shots,),
        in_specs=[pl.BlockSpec((1, LANES), lambda s: (0, 0)), field, side, side, field],
        out_specs=pl.BlockSpec((1, ROWS, blocks, LANES), lambda s: (s, 0, 0, 0)),
        out_shape=jax.ShapeDtypeStruct((shots, ROWS, blocks, LANES), F32),
        name="stats",
    )(mask, multiples, left, right, recorded)

    per_device = -(-shots // trace_count)
    extra = per_device * trace_count - shots
    if extra:
        stats = jnp.pad(stats, ((0, extra), (0, 0), (0, 0), (0, 0)))
    stats = lax.psum_scatter(stats, "trace", scatter_dimension=0, tiled=True)
    stats = lax.all_gather(stats, "freq", axis=0)

    weight = 0.5 * FB * trace_rows * trace_count
    all_blocks = blocks * freq_count
    solved = pl.pallas_call(
        functools.partial(solve_kernel, weight),
        grid=(per_device,),
        in_specs=[pl.BlockSpec((freq_count, 1, ROWS, blocks, LANES), lambda s: (0, s, 0, 0, 0))],
        out_specs=pl.BlockSpec((1, parts, all_blocks, LANES), lambda s: (s, 0, 0, 0)),
        out_shape=jax.ShapeDtypeStruct((per_device, parts, all_blocks, LANES), F32),
        scratch_shapes=[pltpu.VMEM((TAPS, all_blocks, LANES), F32)],
        name="solve",
    )(stats)
    mine = lax.dynamic_slice_in_dim(solved, lax.axis_index("freq") * blocks, blocks, axis=2)
    taps = lax.all_gather(mine, "trace", axis=0, tiled=True)[:shots]

    primaries = pl.pallas_call(
        forward_kernel,
        grid=(shots,),
        in_specs=[pl.BlockSpec((1, parts, blocks, LANES), lambda s: (s, 0, 0, 0)), field, side, side, field],
        out_specs=field,
        out_shape=jax.ShapeDtypeStruct(recorded.shape, F32),
        name="forward",
    )(taps, multiples, left, right, recorded)
    return primaries, taps[..., :TAPS]


def solution(mesh):
    spec = P(None, None, "freq", "trace")
    return jax.shard_map(
        body,
        mesh=mesh,
        in_specs=(spec, spec),
        out_specs=(spec, P(None, None, "freq", None)),
        check_vma=False,
    )
```

```python
import functools

import jax
import jax.numpy as jnp
from jax import lax
from jax.experimental import pallas as pl
from jax.experimental.pallas import tpu as pltpu
from jax.sharding import PartitionSpec as P

FB = 64
TAPS = 64
ITERS = 3
HALF = TAPS // 2
LANES = 128
ROWS = 4 + HALF
F32 = jnp.float32
BF16 = jnp.bfloat16


def lanes_of(shape):
    return lax.broadcasted_iota(jnp.int32, shape, len(shape) - 1)


def turn(value, shift):
    shift = shift % LANES
    return value if shift == 0 else pltpu.roll(value, shift, 1)


def split(value):
    high = value.astype(BF16)
    return high, (value - high.astype(F32)).astype(BF16)


def tiles(m_ref, left_ref, right_ref, b, part):
    group_rows = left_ref.shape[2]
    group, first = (b * FB) // group_rows, (b * FB) % group_rows
    main = m_ref[0, part, b * FB : (b + 1) * FB, :]
    left = turn(left_ref[0, part, first : first + FB, :], LANES - HALF - HALF * group)
    right = turn(right_ref[0, part, first : first + FB, :], -HALF * group)
    lane = lanes_of(main.shape)
    halo = jnp.where(lane < HALF, right, jnp.where(lane >= LANES - HALF, left, 0.0))
    return main, halo


def three(pair):
    (rh, rl), (ih, il) = pair
    return jnp.concatenate([rh, ih, rh, ih, rl, il], 0)


def three_re(pair):
    (rh, rl), (ih, il) = pair
    return jnp.concatenate([rh, ih, rl, il, rh, ih], 0)


def three_im(pair):
    (rh, rl), (ih, il) = pair
    return jnp.concatenate([ih, -rh, il, -rl, ih, -rh], 0)


def over_first(left, right):
    return lax.dot_general(left, right, (((0,), (0,)), ((), ())), preferred_element_type=F32)


def diagonals(main, halo, offset):
    lane = lanes_of((8, LANES))
    total = jnp.zeros((8, LANES), F32)
    for g in range(LANES // 8):
        shift = offset - 8 * g
        own = turn(main[8 * g : 8 * g + 8], shift)
        other = turn(halo[8 * g : 8 * g + 8], shift)
        outside = lane < shift if shift >= 0 else lane >= LANES + shift
        total = total + jnp.where(outside, other, own)
    row = lax.broadcasted_iota(jnp.int32, (8, LANES), 0)
    result = jnp.where(row == 0, total, 0.0)
    for s in range(1, 8):
        result = result + jnp.where(row == s, turn(total, -s), 0.0)
    return jnp.sum(result, axis=0, keepdims=True)


def stats_kernel(mask_ref, m_ref, left_ref, right_ref, rec_ref, out_ref):
    for b in range(m_ref.shape[2] // FB):
        windows, starts, ends, records = [], [], [], []
        for part in range(2):
            main, halo = tiles(m_ref, left_ref, right_ref, b, part)
            turned = turn(main, HALF)
            shifted = jnp.where(lanes_of(main.shape) < HALF, turn(halo, HALF), turned)
            windows.append(split(jnp.concatenate([main, halo], 1)))
            starts.append(split(jnp.concatenate([shifted, rec_ref[0, part, b * FB : (b + 1) * FB, :]], 1)))
            ends.append(split(turned))
        crossed = over_first(three(starts), jnp.concatenate([three_re(windows), three_im(windows)], 1))
        edge = over_first(three(ends)[:, :TAPS], jnp.concatenate([three_re(ends), three_im(ends)], 1))
        quads = []
        for first, offset in ((0, HALF), (LANES, HALF - 1)):
            for column in (0, 2 * LANES):
                rows = slice(first, first + LANES)
                quads.append(
                    diagonals(
                        crossed[rows, column : column + LANES],
                        crossed[rows, column + LANES : column + 2 * LANES],
                        offset,
                    )
                )
        quads[3] = -quads[3]
        real, imag = edge[:, :LANES], turn(edge[:, LANES:], TAPS)
        lane = lanes_of((HALF, LANES))
        corner = jnp.where(
            lane < HALF,
            real[:HALF],
            jnp.where(lane < TAPS, real[HALF:], jnp.where(lane < TAPS + HALF, imag[:HALF], imag[HALF:])),
        )
        corner = jnp.where(mask_ref[...] > 0.0, corner, 0.0)
        out_ref[0, :, b, :] = jnp.concatenate(quads + [corner], 0)


def exact(left, right):
    return jnp.dot(left, right, precision=lax.Precision.HIGHEST, preferred_element_type=F32)


def mirror(total):
    rows = lax.broadcasted_iota(jnp.int32, (LANES, LANES), 0)
    return (rows + lanes_of((LANES, LANES)) == total).astype(F32)


def total_of(value):
    return jnp.sum(jnp.sum(value, axis=1, keepdims=True), axis=0, keepdims=True)


def solve_kernel(weight, st_ref, out_ref, matrix):
    blocks = st_ref.shape[0] * st_ref.shape[3]

    def row(r):
        return st_ref[:, 0, r, :, :].reshape(blocks, LANES)

    lane = lanes_of((blocks, LANES))
    place = lane % TAPS
    is_real = lane < TAPS
    carry_right = place < HALF - 1
    carry_left = place > HALF
    in_right = place < HALF
    right = [None] * HALF
    for i in reversed(range(HALF)):
        value = jnp.where(in_right, row(4 + i), 0.0)
        if i + 1 < HALF:
            value = value + jnp.where(carry_right, turn(right[i + 1], -1), 0.0)
        right[i] = value
        if i >= 1:
            matrix[i - 1] = jnp.where(carry_right, turn(value, -1), 0.0)
    matrix[HALF - 1] = jnp.zeros((blocks, LANES), F32)
    last = None
    for i in range(HALF):
        value = jnp.where(in_right, 0.0, row(4 + i))
        if i:
            value = value + jnp.where(carry_left, turn(last, 1), 0.0)
        last = value
        matrix[HALF + i] = value
    lag_real = jnp.where(is_real, row(0), 0.0) + jnp.where(lane < HALF, right[0], 0.0)
    lag_imag = jnp.where(is_real, row(1), 0.0) + jnp.where(lane < HALF, turn(right[0], TAPS), 0.0)
    back = mirror(LANES)
    toep_real = jnp.where(is_real, lag_real, exact(lag_real, back))
    toep_imag = jnp.where(is_real, -lag_imag, exact(lag_imag, back))
    for t in range(TAPS):
        toep = jnp.where(is_real, turn(toep_real, t), turn(toep_imag, TAPS + t))
        matrix[t] = toep - jnp.where(is_real, matrix[t], -matrix[t])

    gradient = jnp.where(is_real, row(2), turn(row(3), TAPS))
    filters = jnp.zeros((blocks, LANES), F32)
    direction = norm_now = None
    none = jnp.zeros((1, LANES), F32)
    for iteration in range(ITERS):
        norm_next = total_of(gradient * gradient)
        if iteration == 0:
            direction = gradient
        else:
            direction = gradient + (norm_next / norm_now) * direction
        norm_now = norm_next
        by_real = jnp.zeros((blocks, LANES), F32)
        by_imag = jnp.zeros((blocks, LANES), F32)
        for t in range(TAPS):
            by_real = by_real + direction[:, t : t + 1] * matrix[t]
            by_imag = by_imag + direction[:, TAPS + t : TAPS + t + 1] * matrix[t]
        by_imag = turn(by_imag, TAPS)
        normal = by_real + jnp.where(is_real, -by_imag, by_imag)
        before = jnp.concatenate([none, direction[:-1]], 0)
        after = jnp.concatenate([direction[1:], none], 0)
        normal = normal + weight * (2.0 * direction - before - after)
        step_len = norm_now / total_of(direction * normal)
        filters = filters + step_len * direction
        gradient = gradient - step_len * normal
    out_ref[0, 0] = exact(filters, mirror(TAPS - 1))
    out_ref[0, 1] = exact(jnp.where(is_real, 0.0, filters), mirror(2 * TAPS - 1))


def forward_kernel(h_ref, m_ref, left_ref, right_ref, rec_ref, out_ref):
    rows = lax.broadcasted_iota(jnp.int32, (LANES, LANES), 0)
    tap = lanes_of((LANES, LANES)) + HALF - rows
    direct = (tap >= 0) & (tap < TAPS)
    for b in range(m_ref.shape[2] // FB):
        windows, bands = [], []
        for part in range(2):
            windows.append(split(jnp.concatenate(tiles(m_ref, left_ref, right_ref, b, part), 1)))
            base = jnp.where(lanes_of((1, LANES)) < TAPS, h_ref[0, part, b : b + 1, :], 0.0)
            base = pltpu.roll(jnp.broadcast_to(base, (8, LANES)), 0, 1, stride=1, stride_axis=0)
            ring = jnp.concatenate([turn(base, 8 * g - HALF) for g in range(LANES // 8)], 0)
            band = jnp.concatenate([jnp.where(direct, ring, 0.0), jnp.where(direct, 0.0, ring)], 0)
            bands.append(split(band))
        (rh, rl), (ih, il) = windows
        high, low = jnp.concatenate([rh, ih], 1), jnp.concatenate([rl, il], 1)
        sides = []
        for term in range(2):
            real, imag = bands[0][term], bands[1][term]
            sides.append(
                jnp.concatenate(
                    [jnp.concatenate([real, imag], 1), jnp.concatenate([-imag, real], 1)], 0
                )
            )
        both = jnp.dot(jnp.concatenate([high, low], 0), sides[0], preferred_element_type=F32)
        applied = both[:FB] + both[FB:] + jnp.dot(high, sides[1], preferred_element_type=F32)
        span = slice(b * FB, (b + 1) * FB)
        out_ref[0, 0, span, :] = rec_ref[0, 0, span, :] - applied[:, :LANES]
        out_ref[0, 1, span, :] = rec_ref[0, 1, span, :] - applied[:, LANES:]


def packed(value):
    count = LANES // HALF
    return jnp.concatenate(jnp.split(value, count, axis=2), axis=3)


def body(recorded, multiples):
    shots, parts, freq_rows, trace_rows = multiples.shape
    blocks = freq_rows // FB
    trace_count, freq_count = lax.axis_size("trace"), lax.axis_size("freq")
    me = lax.axis_index("trace")
    up = [(i, i + 1) for i in range(trace_count - 1)]
    down = [(j, i) for i, j in up]
    left = lax.ppermute(packed(multiples[..., trace_rows - HALF :]), "trace", up)
    right = lax.ppermute(packed(multiples[..., :HALF]), "trace", down)

    place = jnp.arange(LANES)[None, :] % TAPS < HALF
    mask = jnp.where(place, me == trace_count - 1, me == 0).astype(F32)

    field = pl.BlockSpec((1, parts, freq_rows, trace_rows), lambda s: (s, 0, 0, 0))
    side = pl.BlockSpec((1, parts) + left.shape[2:], lambda s: (s, 0, 0, 0))
    stats = pl.pallas_call(
        stats_kernel,
        grid=(shots,),
        in_specs=[pl.BlockSpec((1, LANES), lambda s: (0, 0)), field, side, side, field],
        out_specs=pl.BlockSpec((1, ROWS, blocks, LANES), lambda s: (s, 0, 0, 0)),
        out_shape=jax.ShapeDtypeStruct((shots, ROWS, blocks, LANES), F32),
        name="stats",
    )(mask, multiples, left, right, recorded)

    per_device = -(-shots // trace_count)
    extra = per_device * trace_count - shots
    if extra:
        stats = jnp.pad(stats, ((0, extra), (0, 0), (0, 0), (0, 0)))
    stats = lax.all_to_all(stats, "trace", split_axis=0, concat_axis=0, tiled=True)
    stats = jnp.sum(stats.reshape((trace_count, per_device) + stats.shape[1:]), axis=0)
    stats = lax.all_gather(stats, "freq", axis=0)

    weight = 0.5 * FB * trace_rows * trace_count
    all_blocks = blocks * freq_count
    solved = pl.pallas_call(
        functools.partial(solve_kernel, weight),
        grid=(per_device,),
        in_specs=[pl.BlockSpec((freq_count, 1, ROWS, blocks, LANES), lambda s: (0, s, 0, 0, 0))],
        out_specs=pl.BlockSpec((1, parts, all_blocks, LANES), lambda s: (s, 0, 0, 0)),
        out_shape=jax.ShapeDtypeStruct((per_device, parts, all_blocks, LANES), F32),
        scratch_shapes=[pltpu.VMEM((TAPS, all_blocks, LANES), F32)],
        name="solve",
    )(stats)
    mine = lax.dynamic_slice_in_dim(solved, lax.axis_index("freq") * blocks, blocks, axis=2)
    taps = lax.all_gather(mine, "trace", axis=0, tiled=True)[:shots]

    primaries = pl.pallas_call(
        forward_kernel,
        grid=(shots,),
        in_specs=[pl.BlockSpec((1, parts, blocks, LANES), lambda s: (s, 0, 0, 0)), field, side, side, field],
        out_specs=field,
        out_shape=jax.ShapeDtypeStruct(recorded.shape, F32),
        name="forward",
    )(taps, multiples, left, right, recorded)
    return primaries, taps[..., :TAPS]


def solution(mesh):
    spec = P(None, None, "freq", "trace")
    return jax.shard_map(
        body,
        mesh=mesh,
        in_specs=(spec, spec),
        out_specs=(spec, P(None, None, "freq", None)),
        check_vma=False,
    )
```

```python
import functools

import jax
import jax.numpy as jnp
from jax import lax
from jax.experimental import pallas as pl
from jax.experimental.pallas import tpu as pltpu
from jax.sharding import PartitionSpec as P

FB = 64
TAPS = 64
ITERS = 3
HALF = TAPS // 2
LANES = 128
ROWS = 4 + HALF
F32 = jnp.float32
BF16 = jnp.bfloat16


def lanes_of(shape):
    return lax.broadcasted_iota(jnp.int32, shape, len(shape) - 1)


def turn(value, shift):
    shift = shift % LANES
    return value if shift == 0 else pltpu.roll(value, shift, 1)


def split(value):
    high = value.astype(BF16)
    return high, (value - high.astype(F32)).astype(BF16)


def tiles(m_ref, left_ref, right_ref, b, part):
    group_rows = left_ref.shape[2]
    group, first = (b * FB) // group_rows, (b * FB) % group_rows
    main = m_ref[0, part, b * FB : (b + 1) * FB, :]
    left = turn(left_ref[0, part, first : first + FB, :], LANES - HALF - HALF * group)
    right = turn(right_ref[0, part, first : first + FB, :], -HALF * group)
    lane = lanes_of(main.shape)
    halo = jnp.where(lane < HALF, right, jnp.where(lane >= LANES - HALF, left, 0.0))
    return main, halo


def three(pair):
    (rh, rl), (ih, il) = pair
    return jnp.concatenate([rh, ih, rh, ih, rl, il], 0)


def three_re(pair):
    (rh, rl), (ih, il) = pair
    return jnp.concatenate([rh, ih, rl, il, rh, ih], 0)


def three_im(pair):
    (rh, rl), (ih, il) = pair
    return jnp.concatenate([ih, -rh, il, -rl, ih, -rh], 0)


def over_first(left, right):
    return lax.dot_general(left, right, (((0,), (0,)), ((), ())), preferred_element_type=F32)


def diagonals(main, halo, offset):
    lane = lanes_of((8, LANES))
    total = jnp.zeros((8, LANES), F32)
    for g in range(LANES // 8):
        shift = offset - 8 * g
        own = turn(main[8 * g : 8 * g + 8], shift)
        other = turn(halo[8 * g : 8 * g + 8], shift)
        outside = lane < shift if shift >= 0 else lane >= LANES + shift
        total = total + jnp.where(outside, other, own)
    row = lax.broadcasted_iota(jnp.int32, (8, LANES), 0)
    result = jnp.where(row == 0, total, 0.0)
    for s in range(1, 8):
        result = result + jnp.where(row == s, turn(total, -s), 0.0)
    return jnp.sum(result, axis=0, keepdims=True)


def stats_kernel(mask_ref, m_ref, left_ref, right_ref, rec_ref, out_ref):
    for b in range(m_ref.shape[2] // FB):
        windows, starts, ends, records = [], [], [], []
        for part in range(2):
            main, halo = tiles(m_ref, left_ref, right_ref, b, part)
            turned = turn(main, HALF)
            shifted = jnp.where(lanes_of(main.shape) < HALF, turn(halo, HALF), turned)
            windows.append(split(jnp.concatenate([main, halo], 1)))
            starts.append(split(jnp.concatenate([shifted, rec_ref[0, part, b * FB : (b + 1) * FB, :]], 1)))
            ends.append(split(turned))
        crossed = over_first(three(starts), jnp.concatenate([three_re(windows), three_im(windows)], 1))
        edge = over_first(three(ends)[:, :TAPS], jnp.concatenate([three_re(ends), three_im(ends)], 1))
        quads = []
        for first, offset in ((0, HALF), (LANES, HALF - 1)):
            for column in (0, 2 * LANES):
                rows = slice(first, first + LANES)
                quads.append(
                    diagonals(
                        crossed[rows, column : column + LANES],
                        crossed[rows, column + LANES : column + 2 * LANES],
                        offset,
                    )
                )
        quads[3] = -quads[3]
        real, imag = edge[:, :LANES], turn(edge[:, LANES:], TAPS)
        lane = lanes_of((HALF, LANES))
        corner = jnp.where(
            lane < HALF,
            real[:HALF],
            jnp.where(lane < TAPS, real[HALF:], jnp.where(lane < TAPS + HALF, imag[:HALF], imag[HALF:])),
        )
        corner = jnp.where(mask_ref[...] > 0.0, corner, 0.0)
        out_ref[0, :, b, :] = jnp.concatenate(quads + [corner], 0)


def exact(left, right):
    return jnp.dot(left, right, precision=lax.Precision.HIGHEST, preferred_element_type=F32)


def mirror(total):
    rows = lax.broadcasted_iota(jnp.int32, (LANES, LANES), 0)
    return (rows + lanes_of((LANES, LANES)) == total).astype(F32)


def total_of(value):
    return jnp.sum(jnp.sum(value, axis=1, keepdims=True), axis=0, keepdims=True)


def solve_kernel(weight, st_ref, out_ref, matrix):
    blocks = st_ref.shape[0] * st_ref.shape[3]

    def row(r):
        return st_ref[:, 0, r, :, :].reshape(blocks, LANES)

    lane = lanes_of((blocks, LANES))
    place = lane % TAPS
    is_real = lane < TAPS
    carry_right = place < HALF - 1
    carry_left = place > HALF
    in_right = place < HALF
    right = [None] * HALF
    for i in reversed(range(HALF)):
        value = jnp.where(in_right, row(4 + i), 0.0)
        if i + 1 < HALF:
            value = value + jnp.where(carry_right, turn(right[i + 1], -1), 0.0)
        right[i] = value
        if i >= 1:
            matrix[i - 1] = jnp.where(carry_right, turn(value, -1), 0.0)
    matrix[HALF - 1] = jnp.zeros((blocks, LANES), F32)
    last = None
    for i in range(HALF):
        value = jnp.where(in_right, 0.0, row(4 + i))
        if i:
            value = value + jnp.where(carry_left, turn(last, 1), 0.0)
        last = value
        matrix[HALF + i] = value
    lag_real = jnp.where(is_real, row(0), 0.0) + jnp.where(lane < HALF, right[0], 0.0)
    lag_imag = jnp.where(is_real, row(1), 0.0) + jnp.where(lane < HALF, turn(right[0], TAPS), 0.0)
    back = mirror(LANES)
    toep_real = jnp.where(is_real, lag_real, exact(lag_real, back))
    toep_imag = jnp.where(is_real, -lag_imag, exact(lag_imag, back))
    for t in range(TAPS):
        toep = jnp.where(is_real, turn(toep_real, t), turn(toep_imag, TAPS + t))
        matrix[t] = toep - jnp.where(is_real, matrix[t], -matrix[t])

    gradient = jnp.where(is_real, row(2), turn(row(3), TAPS))
    filters = jnp.zeros((blocks, LANES), F32)
    direction = norm_now = None
    none = jnp.zeros((1, LANES), F32)
    for iteration in range(ITERS):
        norm_next = total_of(gradient * gradient)
        if iteration == 0:
            direction = gradient
        else:
            direction = gradient + (norm_next / norm_now) * direction
        norm_now = norm_next
        by_real = jnp.zeros((blocks, LANES), F32)
        by_imag = jnp.zeros((blocks, LANES), F32)
        for t in range(TAPS):
            by_real = by_real + direction[:, t : t + 1] * matrix[t]
            by_imag = by_imag + direction[:, TAPS + t : TAPS + t + 1] * matrix[t]
        by_imag = turn(by_imag, TAPS)
        normal = by_real + jnp.where(is_real, -by_imag, by_imag)
        before = jnp.concatenate([none, direction[:-1]], 0)
        after = jnp.concatenate([direction[1:], none], 0)
        normal = normal + weight * (2.0 * direction - before - after)
        step_len = norm_now / total_of(direction * normal)
        filters = filters + step_len * direction
        gradient = gradient - step_len * normal
    out_ref[0, 0] = exact(filters, mirror(TAPS - 1))
    out_ref[0, 1] = exact(jnp.where(is_real, 0.0, filters), mirror(2 * TAPS - 1))


def forward_kernel(h_ref, m_ref, left_ref, right_ref, rec_ref, out_ref):
    rows = lax.broadcasted_iota(jnp.int32, (LANES, LANES), 0)
    tap = lanes_of((LANES, LANES)) + HALF - rows
    direct = (tap >= 0) & (tap < TAPS)
    for b in range(m_ref.shape[2] // FB):
        windows, bands = [], []
        for part in range(2):
            windows.append(split(jnp.concatenate(tiles(m_ref, left_ref, right_ref, b, part), 1)))
            base = jnp.where(lanes_of((1, LANES)) < TAPS, h_ref[0, part, b : b + 1, :], 0.0)
            base = pltpu.roll(jnp.broadcast_to(base, (8, LANES)), 0, 1, stride=1, stride_axis=0)
            ring = jnp.concatenate([turn(base, 8 * g - HALF) for g in range(LANES // 8)], 0)
            band = jnp.concatenate([jnp.where(direct, ring, 0.0), jnp.where(direct, 0.0, ring)], 0)
            bands.append(split(band))
        (rh, rl), (ih, il) = windows
        high, low = jnp.concatenate([rh, ih], 1), jnp.concatenate([rl, il], 1)
        sides = []
        for term in range(2):
            real, imag = bands[0][term], bands[1][term]
            sides.append(
                jnp.concatenate(
                    [jnp.concatenate([real, imag], 1), jnp.concatenate([-imag, real], 1)], 0
                )
            )
        both = jnp.dot(jnp.concatenate([high, low], 0), sides[0], preferred_element_type=F32)
        applied = both[:FB] + both[FB:] + jnp.dot(high, sides[1], preferred_element_type=F32)
        span = slice(b * FB, (b + 1) * FB)
        out_ref[0, 0, span, :] = rec_ref[0, 0, span, :] - applied[:, :LANES]
        out_ref[0, 1, span, :] = rec_ref[0, 1, span, :] - applied[:, LANES:]


def packed(value):
    count = LANES // HALF
    return jnp.concatenate(jnp.split(value, count, axis=2), axis=3)


def shared(value, axis):
    copies = jnp.broadcast_to(value, (lax.axis_size(axis),) + value.shape)
    return lax.all_to_all(copies, axis, split_axis=0, concat_axis=0, tiled=True)


def body(recorded, multiples):
    shots, parts, freq_rows, trace_rows = multiples.shape
    blocks = freq_rows // FB
    trace_count, freq_count = lax.axis_size("trace"), lax.axis_size("freq")
    me = lax.axis_index("trace")
    up = [(i, i + 1) for i in range(trace_count - 1)]
    down = [(j, i) for i, j in up]
    left = lax.ppermute(packed(multiples[..., trace_rows - HALF :]), "trace", up)
    right = lax.ppermute(packed(multiples[..., :HALF]), "trace", down)

    place = jnp.arange(LANES)[None, :] % TAPS < HALF
    mask = jnp.where(place, me == trace_count - 1, me == 0).astype(F32)

    field = pl.BlockSpec((1, parts, freq_rows, trace_rows), lambda s: (s, 0, 0, 0))
    side = pl.BlockSpec((1, parts) + left.shape[2:], lambda s: (s, 0, 0, 0))
    stats = pl.pallas_call(
        stats_kernel,
        grid=(shots,),
        in_specs=[pl.BlockSpec((1, LANES), lambda s: (0, 0)), field, side, side, field],
        out_specs=pl.BlockSpec((1, ROWS, blocks, LANES), lambda s: (s, 0, 0, 0)),
        out_shape=jax.ShapeDtypeStruct((shots, ROWS, blocks, LANES), F32),
        name="stats",
    )(mask, multiples, left, right, recorded)

    per_device = -(-shots // trace_count)
    extra = per_device * trace_count - shots
    if extra:
        stats = jnp.pad(stats, ((0, extra), (0, 0), (0, 0), (0, 0)))
    stats = lax.all_to_all(stats, "trace", split_axis=0, concat_axis=0, tiled=True)
    stats = jnp.sum(stats.reshape((trace_count, per_device) + stats.shape[1:]), axis=0)
    stats = shared(stats, "freq")

    weight = 0.5 * FB * trace_rows * trace_count
    all_blocks = blocks * freq_count
    solved = pl.pallas_call(
        functools.partial(solve_kernel, weight),
        grid=(per_device,),
        in_specs=[pl.BlockSpec((freq_count, 1, ROWS, blocks, LANES), lambda s: (0, s, 0, 0, 0))],
        out_specs=pl.BlockSpec((1, parts, all_blocks, LANES), lambda s: (s, 0, 0, 0)),
        out_shape=jax.ShapeDtypeStruct((per_device, parts, all_blocks, LANES), F32),
        scratch_shapes=[pltpu.VMEM((TAPS, all_blocks, LANES), F32)],
        name="solve",
    )(stats)
    mine = lax.dynamic_slice_in_dim(solved, lax.axis_index("freq") * blocks, blocks, axis=2)
    taps = shared(mine, "trace").reshape((-1,) + mine.shape[1:])[:shots]

    primaries = pl.pallas_call(
        forward_kernel,
        grid=(shots,),
        in_specs=[pl.BlockSpec((1, parts, blocks, LANES), lambda s: (s, 0, 0, 0)), field, side, side, field],
        out_specs=field,
        out_shape=jax.ShapeDtypeStruct(recorded.shape, F32),
        name="forward",
    )(taps, multiples, left, right, recorded)
    return primaries, taps[..., :TAPS]


def solution(mesh):
    spec = P(None, None, "freq", "trace")
    return jax.shard_map(
        body,
        mesh=mesh,
        in_specs=(spec, spec),
        out_specs=(spec, P(None, None, "freq", None)),
        check_vma=False,
    )
```
